64 devices in a mesh: dp: 4 (over x, y), cp: 16 (over z, core).
Axes of the slice: x: 2, y: 2, z: 8, core: 2. Of those that a mesh axis runs over, the one named last changes fastest.
The devices are a block of a 4x4x8 slice.
Arguments:
- hidden: bfloat16 [65536, 4096], P(('dp', 'cp')), parts along dimension 0
- w_q: bfloat16 [4096, 4, 128], replicated
- w_k: bfloat16 [4096, 1, 128], replicated
- w_v: bfloat16 [4096, 1, 128], replicated
- w_o: bfloat16 [4, 128, 4096], replicated
Outputs:
- output: bfloat16 [65536, 4096], P(('dp', 'cp')), parts along dimension 0
There are 4 independent parts. The reference program is written for one: setup_inputs(seed, part) draws one part's arguments, and reference() takes and returns one part's arrays. A program takes and returns all parts, laid end to end along the dimension named above; an argument that names none is the same for every part.
All inputs are finite; a program needn't handle non-finite values.
Results may differ from the reference program's by a relative error of at most 0.00412167.
Values are sent between devices in bfloat16 or wider.
A program may use at most 768 MiB of HBM per device.

```python
import jax
import jax.numpy as jnp
from jax import lax

CP_SIZE = 16
CHUNK = 512
MODEL_DIM = 4096
HEADS = 4
KV_HEADS = 1
HEAD_DIM = 128
WINDOW = 4096
ROPE_BASE = 10000


def setup_inputs(seed: int = 0, part: int = 0) -> dict:
    seq_len = 2 * CP_SIZE * CHUNK
    weight_keys = jax.random.split(jax.random.key(seed), 4)
    part_key = jax.random.fold_in(jax.random.key(seed + 1), part)
    noise_key, chunk_key = jax.random.split(part_key)
    token_noise = jax.random.normal(noise_key, (2 * CP_SIZE, CHUNK, MODEL_DIM), jnp.float32)
    chunk_means = jax.random.normal(chunk_key, (2 * CP_SIZE, 1, MODEL_DIM), jnp.float32)
    natural = 0.6 * token_noise + 0.8 * chunk_means
    stored = jnp.stack([natural[:CP_SIZE], natural[CP_SIZE:][::-1]], axis=1).reshape(seq_len, MODEL_DIM)
    in_scale = MODEL_DIM ** -0.5
    out_scale = (HEADS * HEAD_DIM) ** -0.5
    w_q = jax.random.normal(weight_keys[0], (MODEL_DIM, HEADS, HEAD_DIM), jnp.float32) * in_scale
    w_k = jax.random.normal(weight_keys[1], (MODEL_DIM, KV_HEADS, HEAD_DIM), jnp.float32) * in_scale
    w_v = jax.random.normal(weight_keys[2], (MODEL_DIM, KV_HEADS, HEAD_DIM), jnp.float32) * in_scale
    w_o = jax.random.normal(weight_keys[3], (HEADS, HEAD_DIM, MODEL_DIM), jnp.float32) * out_scale
    return {'hidden': stored.astype(jnp.bfloat16), 'w_q': w_q.astype(jnp.bfloat16), 'w_k': w_k.astype(jnp.bfloat16), 'w_v': w_v.astype(jnp.bfloat16), 'w_o': w_o.astype(jnp.bfloat16)}


def rotate(values, positions, factor):
    half_dim = values.shape[-1] // 2
    inv_freq = 1.0 / (ROPE_BASE ** (jnp.arange(half_dim, dtype=jnp.float32) * (2.0 / values.shape[-1])))
    angles = positions.astype(jnp.float32)[..., None, None] * inv_freq
    cos_part = jnp.cos(angles)
    sin_part = jnp.sin(angles)
    first_half = values[..., :half_dim].astype(jnp.float32)
    second_half = values[..., half_dim:].astype(jnp.float32)
    rotated = jnp.concatenate([first_half * cos_part - second_half * sin_part, second_half * cos_part + first_half * sin_part], axis=-1)
    return (rotated * factor).astype(jnp.bfloat16)


def to_natural(stored):
    blocks = stored.reshape((CP_SIZE, 2, CHUNK) + stored.shape[1:])
    return jnp.concatenate([blocks[:, 0], blocks[::-1, 1]], axis=0).reshape(stored.shape)


def to_stored(natural):
    blocks = natural.reshape((2 * CP_SIZE, CHUNK) + natural.shape[1:])
    return jnp.stack([blocks[:CP_SIZE], blocks[CP_SIZE:][::-1]], axis=1).reshape(natural.shape)


def reference(hidden, w_q, w_k, w_v, w_o):
    seq_len = hidden.shape[0]
    group_size = HEADS // KV_HEADS
    dev_ids = jnp.arange(CP_SIZE)[:, None]
    chunk_ids = jnp.concatenate([dev_ids, 2 * CP_SIZE - 1 - dev_ids], axis=1)
    positions = (chunk_ids[:, :, None] * CHUNK + jnp.arange(CHUNK)).reshape(seq_len)
    q_flat = jnp.dot(hidden, w_q.reshape(MODEL_DIM, HEADS * HEAD_DIM), preferred_element_type=jnp.float32).astype(jnp.bfloat16)
    k_flat = jnp.dot(hidden, w_k.reshape(MODEL_DIM, KV_HEADS * HEAD_DIM), preferred_element_type=jnp.float32).astype(jnp.bfloat16)
    v_flat = jnp.dot(hidden, w_v.reshape(MODEL_DIM, KV_HEADS * HEAD_DIM), preferred_element_type=jnp.float32).astype(jnp.bfloat16)
    q_nat = to_natural(rotate(q_flat.reshape(seq_len, HEADS, HEAD_DIM), positions, HEAD_DIM ** -0.5))
    k_nat = to_natural(rotate(k_flat.reshape(seq_len, KV_HEADS, HEAD_DIM), positions, 1.0))
    v_nat = to_natural(v_flat.reshape(seq_len, KV_HEADS, HEAD_DIM))
    block_rows = min(CHUNK, 128)
    key_span = WINDOW + block_rows
    pad_zeros = jnp.zeros((WINDOW, KV_HEADS, HEAD_DIM), jnp.bfloat16)
    k_pad = jnp.concatenate([pad_zeros, k_nat], axis=0)
    v_pad = jnp.concatenate([pad_zeros, v_nat], axis=0)

    def one_block(block_id):
        row_start = block_id * block_rows
        q_part = lax.dynamic_slice_in_dim(q_nat, row_start, block_rows, axis=0).reshape(block_rows, KV_HEADS, group_size, HEAD_DIM)
        k_part = lax.dynamic_slice_in_dim(k_pad, row_start, key_span, axis=0)
        v_part = lax.dynamic_slice_in_dim(v_pad, row_start, key_span, axis=0)
        q_pos = row_start + jnp.arange(block_rows)
        k_pos = row_start - WINDOW + jnp.arange(key_span)
        allowed = (k_pos[None, :] <= q_pos[:, None]) & (q_pos[:, None] - k_pos[None, :] < WINDOW) & (k_pos[None, :] >= 0)
        scores = jnp.einsum('qkgd,skd->kgqs', q_part.astype(jnp.float32), k_part.astype(jnp.float32))
        scores = jnp.where(allowed, scores, -jnp.inf)
        row_max = jnp.max(scores, axis=-1, keepdims=True)
        exp_scores = jnp.exp(scores - row_max)
        row_sum = jnp.sum(exp_scores, axis=-1)
        attn_out = jnp.einsum('kgqs,skd->qkgd', exp_scores.astype(jnp.bfloat16).astype(jnp.float32), v_part.astype(jnp.float32))
        attn_out = attn_out / jnp.transpose(row_sum, (2, 0, 1))[..., None]
        return attn_out.astype(jnp.bfloat16).reshape(block_rows, HEADS * HEAD_DIM)

    o_nat = lax.map(one_block, jnp.arange(seq_len // block_rows)).reshape(seq_len, HEADS * HEAD_DIM)
    o_stored = to_stored(o_nat)
    return jnp.dot(o_stored, w_o.reshape(HEADS * HEAD_DIM, MODEL_DIM), preferred_element_type=jnp.float32).astype(jnp.bfloat16)
```

```python
import functools

import jax
import jax.numpy as jnp
from jax import lax
from jax.experimental import pallas as pl
from jax.experimental.pallas import tpu as pltpu
from jax.sharding import PartitionSpec as P

WINDOW = 4096
ROPE_BASE = 10000.0
LOG2E = 1.4426950408889634
NEG = -jnp.inf
RB = 256
CORES = 2


def rope_tables(positions, head_dim):
    half_dim = head_dim // 2
    inv_freq = 1.0 / (ROPE_BASE ** (jnp.arange(half_dim, dtype=jnp.float32) * (2.0 / head_dim)))
    angles = positions.astype(jnp.float32)[:, None] * inv_freq
    cos_part = jnp.cos(angles)
    sin_part = jnp.sin(angles)
    return jnp.concatenate([cos_part, cos_part], axis=-1), jnp.concatenate([-sin_part, sin_part], axis=-1)


def rotate(values, cos_part, sin_part):
    return values * cos_part + pltpu.roll(values, values.shape[1] // 2, 1) * sin_part


def flash_block(q, keys, vals, masks, state):
    lanes = q.shape[1]
    tiles = []
    for k_t, mask in zip(keys, masks):
        scores = jnp.dot(q, k_t, preferred_element_type=jnp.float32)
        if mask is not None:
            scores = jnp.where(mask, scores, NEG)
        tiles.append([scores[:, j:j + lanes] for j in range(0, scores.shape[1], lanes)])
    flat = [tile for group in tiles for tile in group]
    peak = functools.reduce(jnp.maximum, flat)
    peak = jnp.broadcast_to(jnp.max(peak, axis=1, keepdims=True), peak.shape)
    if state is not None:
        peak = jnp.maximum(state[0], peak)
    probs = [[jnp.exp2((tile - peak) * LOG2E) for tile in group] for group in tiles]
    total = functools.reduce(jnp.add, [tile for group in probs for tile in group])
    out = None
    for group, v in zip(probs, vals):
        p = jnp.concatenate([tile.astype(jnp.bfloat16) for tile in group], axis=1)
        part = jnp.dot(p, v, preferred_element_type=jnp.float32)
        out = part if out is None else out + part
    if state is not None:
        scale = jnp.exp2((state[0] - peak) * LOG2E)
        total = state[1] * scale + total
        out = state[2] * scale + out
    return peak, total, out


def make_attend(q_s, m_s, l_s, acc_s, kbuf, vbuf, heads, chunk):
    blocks = chunk // RB

    def load_state(n, rows):
        return m_s[n, rows, :], l_s[n, rows, :], acc_s[n, rows, :]

    def store_state(n, rows, state):
        m_s[n, rows, :], l_s[n, rows, :], acc_s[n, rows, :] = state

    def full(n, slots, unroll=2):
        def body(step, _):
            for u in range(unroll):
                rows = pl.ds(pl.multiple_of((step * unroll + u) * RB, RB), RB)
                state = flash_block(q_s[n, rows, :], [kbuf[s] for s in slots], [vbuf[s] for s in slots], [None] * len(slots), load_state(n, rows))
                store_state(n, rows, state)
            return 0
        lax.fori_loop(0, heads * blocks // unroll, body, 0)

    def masked(n, slot, diag):
        row_ids = lax.broadcasted_iota(jnp.int32, (RB, RB), 0)
        col_ids = lax.broadcasted_iota(jnp.int32, (RB, RB), 1)
        tri = (col_ids <= row_ids) if diag else (col_ids > row_ids)

        def body(h, _):
            for tb in range(blocks):
                rows = pl.ds(pl.multiple_of(h * chunk + tb * RB, RB), RB)
                whole = range(0, tb) if diag else range(tb + 1, blocks)
                picks = [(kb, None) for kb in whole] + [(tb, tri)]
                keys = [kbuf[slot, :, kb * RB:(kb + 1) * RB] for kb, _ in picks]
                vals = [vbuf[slot, kb * RB:(kb + 1) * RB, :] for kb, _ in picks]
                state = flash_block(q_s[n, rows, :], keys, vals, [m for _, m in picks], None if diag else load_state(n, rows))
                store_state(n, rows, state)
            return 0
        lax.fori_loop(0, heads, body, 0)

    return full, masked


def fused_kernel(cp_size, rounds, heads, cos_ref, sin_ref, x_hbm, wk_hbm, wv_hbm, wq_hbm, o_ref,
                 xbuf, wkv, wq_raw, wq_f32, wq, q_s, m_s, l_s, acc_s, kbuf, vbuf,
                 x_sem, w_sem, rail_send_sem, rail_recv_sem, sib_send_sem, sib_recv_sem):
    head_dim = q_s.shape[2]
    chunk = vbuf.shape[1]
    chips = cp_size // CORES
    me = lax.axis_index('cp')
    c = me // CORES
    b = me % CORES
    is_last = c == chips - 1
    above, below, sibling = me + CORES, me - CORES, c * CORES + (1 - b)
    has_above, has_below = c < chips - 1, c > 0

    def slot(n, r, s):
        return (n * (rounds + 1) + r) * 2 + s

    wk_copy = pltpu.make_async_copy(wk_hbm, wkv.at[:, :head_dim], w_sem.at[0])
    wv_copy = pltpu.make_async_copy(wv_hbm, wkv.at[:, head_dim:], w_sem.at[1])
    wq_copy = pltpu.make_async_copy(wq_hbm, wq_raw, w_sem.at[2])
    tiles = x_hbm.shape[0] // RB
    x_copies = [pltpu.make_async_copy(x_hbm.at[pl.ds(t * RB, RB)], xbuf.at[pl.ds(t * RB, RB)], x_sem.at[t]) for t in range(tiles)]
    wk_copy.start()
    wv_copy.start()
    for copy in x_copies:
        copy.start()
    wq_copy.start()

    barrier = pltpu.get_barrier_semaphore()
    pl.semaphore_signal(barrier, inc=1, device_id={'cp': sibling}, device_id_type=pl.DeviceIdType.MESH)

    @pl.when(has_above)
    def _():
        pl.semaphore_signal(barrier, inc=1, device_id={'cp': above}, device_id_type=pl.DeviceIdType.MESH)

    @pl.when(has_below)
    def _():
        pl.semaphore_signal(barrier, inc=1, device_id={'cp': below}, device_id_type=pl.DeviceIdType.MESH)

    bufs = (kbuf, vbuf)

    def rail(n, r, kv):
        if n == 0:
            src, cond, target = slot(0, r - 1, 0), has_above & (c >= r - 1), above
        else:
            src = slot(1, 0, 0) if r == 1 else jnp.where(is_last, slot(0, r - 2, 0), slot(1, r - 1, 0))
            cond, target = has_below, below
        return cond, pltpu.make_async_remote_copy(
            src_ref=bufs[kv].at[src], dst_ref=bufs[kv].at[slot(n, r, 0)],
            send_sem=rail_send_sem.at[n, r - 1, kv], recv_sem=rail_recv_sem.at[n, r - 1, kv],
            device_id={'cp': target}, device_id_type=pl.DeviceIdType.MESH)

    def arrives(n, r):
        return c >= r if n == 0 else has_above

    def sib(n, r, kv):
        return pltpu.make_async_remote_copy(
            src_ref=bufs[kv].at[slot(n, r, 0)], dst_ref=bufs[kv].at[slot(n, r, 1)],
            send_sem=sib_send_sem.at[n, r, kv], recv_sem=sib_recv_sem.at[n, r, kv],
            device_id={'cp': sibling}, device_id_type=pl.DeviceIdType.MESH)

    own_push = ((b == 0) | is_last, b == 1)
    own_take = ((b == 1) | is_last, b == 0)

    def start_rail(n, r, kv):
        cond, copy = rail(n, r, kv)
        pl.when(cond)(copy.start)

    def relay(n, r, kv):
        @pl.when(arrives(n, r))
        def _():
            rail(n, r, kv)[1].wait_recv()
            sib(n, r, kv).start()
        if r < rounds:
            start_rail(n, r + 1, kv)

    def take_sib(n, r):
        cond = own_take[n] if r == 0 else arrives(n, r)

        @pl.when(cond)
        def _():
            for kv in range(2):
                sib(n, r, kv).wait_recv()

    full, masked = make_attend(q_s, m_s, l_s, acc_s, kbuf, vbuf, heads, chunk)

    def project_kv(n):
        for tb in range(chunk // RB):
            t = n * (chunk // RB) + tb
            x_copies[t].wait()
            rows = pl.ds(t * RB, RB)
            kv = jnp.dot(xbuf[rows, :], wkv[...], preferred_element_type=jnp.float32).astype(jnp.bfloat16)
            k = rotate(kv[:, :head_dim].astype(jnp.float32), cos_ref[rows, :], sin_ref[rows, :])
            kbuf[slot(n, 0, 0), :, tb * RB:(tb + 1) * RB] = k.T.astype(jnp.bfloat16)
            vbuf[slot(n, 0, 0), tb * RB:(tb + 1) * RB, :] = kv[:, head_dim:]

    wk_copy.wait()
    wv_copy.wait()
    project_kv(0)
    pl.semaphore_wait(barrier, 1 + has_above.astype(jnp.int32) + has_below.astype(jnp.int32))
    for n in range(2):
        if n == 1:
            project_kv(1)
        for kv in range(2):
            start_rail(n, 1, kv)
        @pl.when(own_push[n])
        def _(n=n):
            for kv in range(2):
                sib(n, 0, kv).start()

    wq_copy.wait()
    depth = wq.shape[0]
    span = wq_f32.shape[0] // heads

    def unpack(step, _):
        wq_f32[...] = wq_raw[pl.ds(pl.multiple_of(step * span * heads, span * heads), span * heads), :].astype(jnp.float32)
        for h in range(heads):
            wq[pl.ds(pl.multiple_of(step * span, span), span), h * head_dim:(h + 1) * head_dim] = wq_f32[pl.ds(h, span, stride=heads), :].astype(jnp.bfloat16)
        return 0
    lax.fori_loop(0, depth // span, unpack, 0)

    def project_q(t, _):
        rows = pl.ds(pl.multiple_of(t * RB, RB), RB)
        n = t // (chunk // RB)
        tb = t % (chunk // RB)
        for h in range(heads):
            qh = jnp.dot(xbuf[rows, :], wq[:, h * head_dim:(h + 1) * head_dim], preferred_element_type=jnp.float32).astype(jnp.bfloat16).astype(jnp.float32)
            qh = rotate(qh, cos_ref[rows, :], sin_ref[rows, :]) * (head_dim ** -0.5)
            q_s[n, pl.ds(pl.multiple_of(h * chunk + tb * RB, RB), RB), :] = qh.astype(jnp.bfloat16)
        return 0
    lax.fori_loop(0, tiles, project_q, 0)

    masked(0, slot(0, 0, 0), True)
    masked(1, slot(1, 0, 0), True)
    take_sib(0, 0)
    take_sib(1, 0)

    @pl.when(b == 1)
    def _():
        full(0, [slot(0, 0, 1)])

    @pl.when(b == 0)
    def _():
        full(1, [slot(1, 0, 1)])

    def pair(n, r):
        take_sib(n, r)
        if n == 0:
            @pl.when(c >= r)
            def _():
                full(0, [slot(0, r, 0), slot(0, r, 1)])
        else:
            full(1, [jnp.where(is_last, slot(0, r - 1, s), slot(1, r, s)) for s in range(2)])

    def edge(n):
        r = rounds
        take_sib(n, r)
        if n == 0:
            @pl.when(c >= r)
            def _():
                masked(0, slot(0, r, 0), False)

                @pl.when(b == 0)
                def _():
                    full(0, [slot(0, r, 1)])
        else:
            flip = (c > chips - 1 - r).astype(jnp.int32)
            base = jnp.where(is_last, slot(0, r - 1, 0), slot(1, r, 0))
            masked(1, base + flip, False)

            @pl.when(b == 1)
            def _():
                full(1, [base + 1 - flip])

    for r in range(1, rounds + 1):
        relay(0, r, 0)
        relay(1, r, 0)
        if r > 1:
            pair(0, r - 1)
        relay(0, r, 1)
        relay(1, r, 1)
        if r > 1:
            pair(1, r - 1)
    for n in range(2):
        edge(n)

    def finish(h, _):
        for n in range(2):
            rows = pl.ds(pl.multiple_of(h * chunk, chunk), chunk)
            total = jnp.sum(l_s[n, rows, :], axis=1, keepdims=True)
            o_ref[n * chunk:(n + 1) * chunk, pl.ds(pl.multiple_of(h * head_dim, head_dim), head_dim)] = (acc_s[n, rows, :] / total).astype(jnp.bfloat16)
        return 0
    lax.fori_loop(0, heads, finish, 0)

    for n in range(2):
        for kv in range(2):
            for r in range(1, rounds + 1):
                cond, copy = rail(n, r, kv)
                pl.when(cond)(copy.wait_send)
                pl.when(arrives(n, r))(sib(n, r, kv).wait_send)
            pl.when(own_push[n])(sib(n, 0, kv).wait_send)


def out_kernel(o_ref, w_ref, y_ref):
    y_ref[...] = jnp.dot(o_ref[...], w_ref[...], preferred_element_type=jnp.float32).astype(jnp.bfloat16)


def solution(mesh):
    cp_size = mesh.shape['cp']

    def device_step(hidden, w_q, w_k, w_v, w_o):
        rows, model_dim = hidden.shape
        chunk = rows // 2
        heads, head_dim = w_q.shape[1], w_q.shape[2]
        rounds = WINDOW // chunk // 2
        me = lax.axis_index('cp')
        chunk_ids = jnp.stack([me, 2 * cp_size - 1 - me])
        positions = (chunk_ids[:, None] * chunk + jnp.arange(chunk)[None, :]).reshape(rows)
        cos_part, sin_part = rope_tables(positions, head_dim)
        slots = 2 * (rounds + 1) * 2
        vmem = pl.BlockSpec(memory_space=pltpu.VMEM)
        hbm = pl.BlockSpec(memory_space=pl.ANY)
        attended = pl.pallas_call(
            functools.partial(fused_kernel, cp_size, rounds, heads),
            out_shape=jax.ShapeDtypeStruct((rows, heads * head_dim), jnp.bfloat16),
            in_specs=[vmem, vmem, hbm, hbm, hbm, hbm],
            out_specs=vmem,
            scratch_shapes=[
                pltpu.VMEM((rows, model_dim), jnp.bfloat16),
                pltpu.VMEM((model_dim, 2 * head_dim), jnp.bfloat16),
                pltpu.VMEM((model_dim * heads, head_dim), jnp.bfloat16),
                pltpu.VMEM((512 * heads, head_dim), jnp.float32),
                pltpu.VMEM((model_dim, heads * head_dim), jnp.bfloat16),
                pltpu.VMEM((2, heads * chunk, head_dim), jnp.bfloat16),
                pltpu.VMEM((2, heads * chunk, head_dim), jnp.float32),
                pltpu.VMEM((2, heads * chunk, head_dim), jnp.float32),
                pltpu.VMEM((2, heads * chunk, head_dim), jnp.float32),
                pltpu.VMEM((slots, head_dim, chunk), jnp.bfloat16),
                pltpu.VMEM((slots, chunk, head_dim), jnp.bfloat16),
                pltpu.SemaphoreType.DMA((rows // RB,)),
                pltpu.SemaphoreType.DMA((3,)),
                pltpu.SemaphoreType.DMA((2, rounds, 2)),
                pltpu.SemaphoreType.DMA((2, rounds, 2)),
                pltpu.SemaphoreType.DMA((2, rounds + 1, 2)),
                pltpu.SemaphoreType.DMA((2, rounds + 1, 2)),
            ],
            compiler_params=pltpu.CompilerParams(collective_id=0, has_side_effects=True, vmem_limit_bytes=60 << 20),
        )(cos_part, sin_part, hidden, w_k.reshape(model_dim, head_dim), w_v.reshape(model_dim, head_dim), w_q.reshape(model_dim * heads, head_dim))
        width = 512
        return pl.pallas_call(
            out_kernel,
            out_shape=jax.ShapeDtypeStruct((rows, model_dim), jnp.bfloat16),
            grid=(model_dim // width,),
            in_specs=[pl.BlockSpec((rows, heads * head_dim), lambda j: (0, 0)), pl.BlockSpec((heads * head_dim, width), lambda j: (0, j))],
            out_specs=pl.BlockSpec((rows, width), lambda j: (0, j)),
        )(attended, w_o.reshape(heads * head_dim, model_dim))

    return jax.shard_map(device_step, mesh=mesh, in_specs=(P(('dp', 'cp'), None), P(), P(), P(), P()), out_specs=P(('dp', 'cp'), None), check_vma=False)
```

```python
import functools

import jax
import jax.numpy as jnp
from jax import lax
from jax.experimental import pallas as pl
from jax.experimental.pallas import tpu as pltpu
from jax.sharding import PartitionSpec as P

WINDOW = 4096
ROPE_BASE = 10000.0
LOG2E = 1.4426950408889634
RB = 256
SUB = 8
CORES = 2


def rope_tables(positions, head_dim):
    half_dim = head_dim // 2
    inv_freq = 1.0 / (ROPE_BASE ** (jnp.arange(half_dim, dtype=jnp.float32) * (2.0 / head_dim)))
    angles = positions.astype(jnp.float32)[:, None] * inv_freq
    cos_part = jnp.cos(angles)
    sin_part = jnp.sin(angles)
    return jnp.concatenate([cos_part, cos_part], axis=-1), jnp.concatenate([-sin_part, sin_part], axis=-1)


def rotate(values, cos_part, sin_part):
    return values * cos_part + pltpu.roll(values, values.shape[1] // 2, 1) * sin_part


def score_part(q, keys, mask, s_ref, row, peak):
    scores = jnp.dot(keys, q, preferred_element_type=jnp.float32)
    if mask is not None:
        scores = jnp.where(mask, scores, -jnp.inf)
    rows = scores.shape[0]
    s_ref[row:row + rows, :] = scores
    top = jnp.max(scores.reshape(rows // SUB, SUB, RB), axis=0)
    return top if peak is None else jnp.maximum(peak, top)


def value_part(s_ref, row, vals, peak, total):
    rows = vals.shape[1]
    probs = jnp.exp2((s_ref[row:row + rows, :].reshape(rows // SUB, SUB, RB) - peak[None]) * LOG2E)
    total = total + jnp.sum(probs, axis=0)
    out = jnp.dot(vals, probs.reshape(rows, RB).astype(jnp.bfloat16), preferred_element_type=jnp.float32)
    return total, out


class Step:
    def __init__(self, node, full=(), diag=None, edge=None):
        self.node, self.full, self.diag, self.edge = node, full, diag, edge

    def parts(self, tb, blocks):
        found = []
        size = blocks * RB
        if self.diag is not None:
            if tb:
                found.append((self.diag, 0, tb * RB, None))
            found.append((self.diag, tb * RB, (tb + 1) * RB, 'le'))
        if self.edge is not None:
            found.append((self.edge, tb * RB, (tb + 1) * RB, 'gt'))
            if tb + 1 < blocks:
                found.append((self.edge, (tb + 1) * RB, size, None))
        for s in self.full:
            found.append((s, 0, size, None))
        return found


def fused_kernel(cp_size, rounds, heads, cos_ref, sin_ref, x_hbm, wk_hbm, wv_hbm, wq_hbm, o_ref,
                 xbuf, wkv, wq_raw, wq_f32, wq, q_s, m_s, l_s, acc_s, kbuf, vbuf,
                 x_sem, w_sem, rail_send_sem, rail_recv_sem, sib_send_sem, sib_recv_sem, *score_refs):
    head_dim = q_s.shape[1]
    chunk = kbuf.shape[1]
    blocks = chunk // RB
    count = heads * blocks
    chips = cp_size // CORES
    me = lax.axis_index('cp')
    c = me // CORES
    b = me % CORES
    is_last = c == chips - 1
    above, below, sibling = me + CORES, me - CORES, c * CORES + (1 - b)
    has_above, has_below = c < chips - 1, c > 0
    s_refs = (score_refs[:count], score_refs[count:2 * count])
    x_refs = (score_refs[2 * count:3 * count], score_refs[3 * count:])

    def slot(n, r, s):
        return (n * (rounds + 1) + r) * 2 + s

    wk_copy = pltpu.make_async_copy(wk_hbm, wkv.at[:, :head_dim], w_sem.at[0])
    wv_copy = pltpu.make_async_copy(wv_hbm, wkv.at[:, head_dim:], w_sem.at[1])
    wq_copy = pltpu.make_async_copy(wq_hbm, wq_raw, w_sem.at[2])
    tiles = x_hbm.shape[0] // RB
    x_copies = [pltpu.make_async_copy(x_hbm.at[pl.ds(t * RB, RB)], xbuf.at[pl.ds(t * RB, RB)], x_sem.at[t]) for t in range(tiles)]
    wk_copy.start()
    wv_copy.start()
    for copy in x_copies:
        copy.start()
    wq_copy.start()

    m_s[...] = jnp.full_like(m_s, -jnp.inf)
    l_s[...] = jnp.zeros_like(l_s)
    acc_s[...] = jnp.zeros_like(acc_s)

    barrier = pltpu.get_barrier_semaphore()
    pl.semaphore_signal(barrier, inc=1, device_id={'cp': sibling}, device_id_type=pl.DeviceIdType.MESH)

    @pl.when(has_above)
    def _():
        pl.semaphore_signal(barrier, inc=1, device_id={'cp': above}, device_id_type=pl.DeviceIdType.MESH)

    @pl.when(has_below)
    def _():
        pl.semaphore_signal(barrier, inc=1, device_id={'cp': below}, device_id_type=pl.DeviceIdType.MESH)

    bufs = (kbuf, vbuf)

    def rail(n, r, kv):
        if n == 0:
            src, cond, target = slot(0, r - 1, 0), has_above & (c >= r - 1), above
        else:
            src = slot(1, 0, 0) if r == 1 else jnp.where(is_last, slot(0, r - 2, 0), slot(1, r - 1, 0))
            cond, target = has_below, below
        return cond, pltpu.make_async_remote_copy(
            src_ref=bufs[kv].at[src], dst_ref=bufs[kv].at[slot(n, r, 0)],
            send_sem=rail_send_sem.at[n, r - 1, kv], recv_sem=rail_recv_sem.at[n, r - 1, kv],
            device_id={'cp': target}, device_id_type=pl.DeviceIdType.MESH)

    def arrives(n, r):
        return c >= r if n == 0 else has_above

    def sib(n, r, kv):
        return pltpu.make_async_remote_copy(
            src_ref=bufs[kv].at[slot(n, r, 0)], dst_ref=bufs[kv].at[slot(n, r, 1)],
            send_sem=sib_send_sem.at[n, r, kv], recv_sem=sib_recv_sem.at[n, r, kv],
            device_id={'cp': sibling}, device_id_type=pl.DeviceIdType.MESH)

    own_push = ((b == 0) | is_last, b == 1)
    own_take = ((b == 1) | is_last, b == 0)

    def start_rail(n, r, kv):
        cond, copy = rail(n, r, kv)
        pl.when(cond)(copy.start)

    def relay(n, r, kv):
        @pl.when(arrives(n, r))
        def _():
            rail(n, r, kv)[1].wait_recv()
            sib(n, r, kv).start()
        if r < rounds:
            start_rail(n, r + 1, kv)

    def project_kv(n):
        for tb in range(blocks):
            t = n * blocks + tb
            x_copies[t].wait()
            rows = pl.ds(t * RB, RB)
            kv = jnp.dot(xbuf[rows, :], wkv[...], preferred_element_type=jnp.float32).astype(jnp.bfloat16).astype(jnp.float32)
            k = rotate(kv[:, :head_dim], cos_ref[rows, :], sin_ref[rows, :])
            kbuf[slot(n, 0, 0), tb * RB:(tb + 1) * RB, :] = k.astype(jnp.bfloat16)
            vbuf[slot(n, 0, 0), :, tb * RB:(tb + 1) * RB] = kv[:, head_dim:].T.astype(jnp.bfloat16)

    wk_copy.wait()
    wv_copy.wait()
    project_kv(0)
    pl.semaphore_wait(barrier, 1 + has_above.astype(jnp.int32) + has_below.astype(jnp.int32))
    for n in range(2):
        if n == 1:
            project_kv(1)
        for kv in range(2):
            start_rail(n, 1, kv)

        @pl.when(own_push[n])
        def _(n=n):
            for kv in range(2):
                sib(n, 0, kv).start()

    wq_copy.wait()
    depth = wq.shape[0]
    span = wq_f32.shape[0] // heads

    def unpack(step, _):
        wq_f32[...] = wq_raw[pl.ds(pl.multiple_of(step * span * heads, span * heads), span * heads), :].astype(jnp.float32)
        for h in range(heads):
            wq[pl.ds(pl.multiple_of(step * span, span), span), h * head_dim:(h + 1) * head_dim] = wq_f32[pl.ds(h, span, stride=heads), :].astype(jnp.bfloat16)
        return 0
    lax.fori_loop(0, depth // span, unpack, 0)

    def project_q(t, _):
        rows = pl.ds(pl.multiple_of(t * RB, RB), RB)
        n = t // blocks
        tb = t % blocks
        q = jnp.dot(xbuf[rows, :], wq[...], preferred_element_type=jnp.float32).astype(jnp.bfloat16).astype(jnp.float32)
        for h in range(heads):
            qh = rotate(q[:, h * head_dim:(h + 1) * head_dim], cos_ref[rows, :], sin_ref[rows, :]) * (head_dim ** -0.5)
            q_s[n, :, pl.ds(pl.multiple_of(h * chunk + tb * RB, RB), RB)] = qh.T.astype(jnp.bfloat16)
        return 0
    lax.fori_loop(0, tiles, project_q, 0)

    key_ids = lax.broadcasted_iota(jnp.int32, (RB, RB), 0)
    query_ids = lax.broadcasted_iota(jnp.int32, (RB, RB), 1)

    def mask_of(kind):
        return None if kind is None else (key_ids <= query_ids if kind == 'le' else key_ids > query_ids)

    def region(values, scores, parity):
        for i in range(count):
            cols = slice(i * RB, (i + 1) * RB)
            s_parts = scores.parts(i % blocks, blocks) if scores is not None else []
            v_parts = values.parts(i % blocks, blocks) if values is not None else []
            if values is not None:
                n = values.node
                m_old = m_s[n, :, cols]
                peak = jnp.maximum(m_old, jnp.broadcast_to(jnp.max(x_refs[parity][i][...], axis=0, keepdims=True), m_old.shape))
                scale = jnp.exp2((m_old - peak) * LOG2E)
                total = l_s[n, :, cols] * scale
            out = top = None
            s_row = v_row = 0
            for j in range(max(len(s_parts), len(v_parts))):
                if j < len(s_parts):
                    at, lo, hi, kind = s_parts[j]
                    top = score_part(q_s[scores.node, :, cols], kbuf[at, lo:hi, :], mask_of(kind), s_refs[1 - parity][i], s_row, top)
                    s_row += hi - lo
                if j < len(v_parts):
                    at, lo, hi, kind = v_parts[j]
                    total, part = value_part(s_refs[parity][i], v_row, vbuf[at, :, lo:hi], peak, total)
                    out = part if out is None else out + part
                    v_row += hi - lo
            if scores is not None:
                x_refs[1 - parity][i][...] = top
            if values is not None:
                m_s[n, :, cols] = peak
                l_s[n, :, cols] = total
                acc_s[n, :, cols] = (acc_s[n, :, cols].reshape(head_dim // SUB, SUB, RB) * scale[None]).reshape(head_dim, RB) + out

    def pair_slots(n, r):
        if n == 0:
            return [slot(0, r, s) for s in range(2)]
        return [jnp.where(is_last, slot(0, r - 1, s), slot(1, r, s)) for s in range(2)]

    one_n, two_n = 1 - b, b
    flip = (c > chips - 1 - rounds).astype(jnp.int32)
    high = jnp.where(is_last, slot(0, rounds - 1, 0), slot(1, rounds, 0))
    low = slot(0, rounds, 0)

    def edge_slots(node):
        return jnp.where(node == 0, low, high + flip), jnp.where(node == 0, low + 1, high + 1 - flip)

    def reaches(node):
        return (node == 1) | (c >= rounds)

    always = me != cp_size
    steps = [
        (Step(two_n, diag=slot(0, 0, 0) + two_n * slot(1, 0, 0)), always),
        (Step(one_n, diag=slot(0, 0, 0) + one_n * slot(1, 0, 0), full=[slot(0, 0, 1) + one_n * slot(1, 0, 0)]), always),
    ]
    for r in range(1, rounds):
        for n in range(2):
            steps.append((Step(n, full=pair_slots(n, r)), (c >= r) if n == 0 else always))
    near, far = edge_slots(two_n), edge_slots(one_n)
    steps.append((Step(two_n, edge=near[0], full=[near[1]]), reaches(two_n)))
    steps.append((Step(one_n, edge=far[0]), reaches(one_n)))

    def relay_both(r, kv):
        for n in range(2):
            relay(n, r, kv)

    def take(n, r, kv):
        cond = own_take[n] if r == 0 else arrives(n, r)
        pl.when(cond)(sib(n, r, kv).wait_recv)

    before = [[] for _ in steps]
    before[0] += [('relay', 1, 0), ('take', 0, 0, 0), ('take', 1, 0, 0)]
    before[1] += [('relay', 1, 1), ('take', 0, 0, 1), ('take', 1, 0, 1), ('take', 0, 1, 0)]
    for r in range(1, rounds):
        at = 2 * r
        before[at] += [('relay', r + 1, 0), ('take', 0, r, 1), ('take', 1, r, 0)]
        before[at + 1] += [('relay', r + 1, 1), ('take', 1, r, 1), ('take', 0, r + 1, 0)]
    before[2 * rounds - 1] += [('take', 1, rounds, 0)]
    before[2 * rounds] += [('take', 0, rounds, 1), ('take', 1, rounds, 1)]

    region(None, steps[0][0], 1)
    for i, (step, valid) in enumerate(steps):
        for what, *args in before[i]:
            (relay_both if what == 'relay' else take)(*args)
        following = steps[i + 1][0] if i + 1 < len(steps) else None
        pl.when(valid)(functools.partial(region, step, following, i % 2))
        if valid is not always and following is not None:
            pl.when(jnp.logical_not(valid))(functools.partial(region, None, following, i % 2))

    def finish(h, _):
        for n in range(2):
            cols = pl.ds(pl.multiple_of(h * chunk, chunk), chunk)
            total = jnp.sum(l_s[n, :, cols], axis=0, keepdims=True)
            o_ref[n * chunk:(n + 1) * chunk, pl.ds(pl.multiple_of(h * head_dim, head_dim), head_dim)] = (acc_s[n, :, cols] / total).T.astype(jnp.bfloat16)
        return 0
    lax.fori_loop(0, heads, finish, 0)

    for n in range(2):
        for kv in range(2):
            for r in range(1, rounds + 1):
                cond, copy = rail(n, r, kv)
                pl.when(cond)(copy.wait_send)
                pl.when(arrives(n, r))(sib(n, r, kv).wait_send)
            pl.when(own_push[n])(sib(n, 0, kv).wait_send)


def out_kernel(o_ref, w_ref, y_ref):
    y_ref[...] = jnp.dot(o_ref[...], w_ref[...], preferred_element_type=jnp.float32).astype(jnp.bfloat16)


def solution(mesh):
    cp_size = mesh.shape['cp']

    def device_step(hidden, w_q, w_k, w_v, w_o):
        rows, model_dim = hidden.shape
        chunk = rows // 2
        heads, head_dim = w_q.shape[1], w_q.shape[2]
        rounds = WINDOW // chunk // 2
        me = lax.axis_index('cp')
        chunk_ids = jnp.stack([me, 2 * cp_size - 1 - me])
        positions = (chunk_ids[:, None] * chunk + jnp.arange(chunk)[None, :]).reshape(rows)
        cos_part, sin_part = rope_tables(positions, head_dim)
        slots = 2 * (rounds + 1) * 2
        vmem = pl.BlockSpec(memory_space=pltpu.VMEM)
        hbm = pl.BlockSpec(memory_space=pl.ANY)
        attended = pl.pallas_call(
            functools.partial(fused_kernel, cp_size, rounds, heads),
            out_shape=jax.ShapeDtypeStruct((rows, heads * head_dim), jnp.bfloat16),
            in_specs=[vmem, vmem, hbm, hbm, hbm, hbm],
            out_specs=vmem,
            scratch_shapes=[
                pltpu.VMEM((rows, model_dim), jnp.bfloat16),
                pltpu.VMEM((model_dim, 2 * head_dim), jnp.bfloat16),
                pltpu.VMEM((model_dim * heads, head_dim), jnp.bfloat16),
                pltpu.VMEM((512 * heads, head_dim), jnp.float32),
                pltpu.VMEM((model_dim, heads * head_dim), jnp.bfloat16),
                pltpu.VMEM((2, head_dim, heads * chunk), jnp.bfloat16),
                pltpu.VMEM((2, SUB, heads * chunk), jnp.float32),
                pltpu.VMEM((2, SUB, heads * chunk), jnp.float32),
                pltpu.VMEM((2, head_dim, heads * chunk), jnp.float32),
                pltpu.VMEM((slots, chunk, head_dim), jnp.bfloat16),
                pltpu.VMEM((slots, head_dim, chunk), jnp.bfloat16),
                pltpu.SemaphoreType.DMA((rows // RB,)),
                pltpu.SemaphoreType.DMA((3,)),
                pltpu.SemaphoreType.DMA((2, rounds, 2)),
                pltpu.SemaphoreType.DMA((2, rounds, 2)),
                pltpu.SemaphoreType.DMA((2, rounds + 1, 2)),
                pltpu.SemaphoreType.DMA((2, rounds + 1, 2)),
            ] + [pltpu.VMEM((2 * chunk, RB), jnp.float32)] * (2 * heads * chunk // RB) + [pltpu.VMEM((SUB, RB), jnp.float32)] * (2 * heads * chunk // RB),
            compiler_params=pltpu.CompilerParams(collective_id=0, has_side_effects=True, vmem_limit_bytes=60 << 20),
        )(cos_part, sin_part, hidden, w_k.reshape(model_dim, head_dim), w_v.reshape(model_dim, head_dim), w_q.reshape(model_dim * heads, head_dim))
        band = 256
        return pl.pallas_call(
            out_kernel,
            out_shape=jax.ShapeDtypeStruct((rows, model_dim), jnp.bfloat16),
            grid=(rows // band,),
            in_specs=[pl.BlockSpec((band, heads * head_dim), lambda j: (j, 0)), vmem],
            out_specs=pl.BlockSpec((band, model_dim), lambda j: (j, 0)),
        )(attended, w_o.reshape(heads * head_dim, model_dim))

    return jax.shard_map(device_step, mesh=mesh, in_specs=(P(('dp', 'cp'), None), P(), P(), P(), P()), out_specs=P(('dp', 'cp'), None), check_vma=False)
```

```python
import functools

import jax
import jax.numpy as jnp
from jax import lax
from jax.experimental import pallas as pl
from jax.experimental.pallas import tpu as pltpu
from jax.sharding import PartitionSpec as P

WINDOW = 4096
ROPE_BASE = 10000.0
LOG2E = 1.4426950408889634
RB = 256
SUB = 8
CORES = 2


def rope_tables(positions, head_dim):
    half_dim = head_dim // 2
    inv_freq = 1.0 / (ROPE_BASE ** (jnp.arange(half_dim, dtype=jnp.float32) * (2.0 / head_dim)))
    angles = inv_freq[:, None] * positions.astype(jnp.float32)[None, :]
    return jnp.cos(angles), jnp.sin(angles)


def rotate(values, cos_part, sin_part):
    half_dim = values.shape[0] // 2
    first, second = values[:half_dim], values[half_dim:]
    return jnp.concatenate([first * cos_part - second * sin_part, second * cos_part + first * sin_part], axis=0)


def score_part(q, keys, mask, s_ref, row, peak):
    scores = jnp.dot(keys, q, preferred_element_type=jnp.float32)
    if mask is not None:
        scores = jnp.where(mask, scores, -jnp.inf)
    rows = scores.shape[0]
    s_ref[row:row + rows, :] = scores
    top = jnp.max(scores.reshape(rows // SUB, SUB, RB), axis=0)
    return top if peak is None else jnp.maximum(peak, top)


def value_part(s_ref, row, vals, peak, total):
    rows = vals.shape[1]
    probs = jnp.exp2((s_ref[row:row + rows, :].reshape(rows // SUB, SUB, RB) - peak[None]) * LOG2E)
    total = total + jnp.sum(probs, axis=0)
    out = jnp.dot(vals, probs.reshape(rows, RB).astype(jnp.bfloat16), preferred_element_type=jnp.float32)
    return total, out


class Step:
    def __init__(self, node, full=(), diag=None, edge=None):
        self.node, self.full, self.diag, self.edge = node, full, diag, edge

    def parts(self, tb, blocks):
        found = []
        size = blocks * RB
        if self.diag is not None:
            if tb:
                found.append((self.diag, 0, tb * RB, None))
            found.append((self.diag, tb * RB, (tb + 1) * RB, 'le'))
        if self.edge is not None:
            found.append((self.edge, tb * RB, (tb + 1) * RB, 'gt'))
            if tb + 1 < blocks:
                found.append((self.edge, (tb + 1) * RB, size, None))
        for s in self.full:
            found.append((s, 0, size, None))
        return found


def fused_kernel(cp_size, rounds, heads, cos_ref, sin_ref, x_hbm, wk_hbm, wv_hbm, wq_hbm, o_ref,
                 xbuf, wk, wv, wq_raw, wq_f32, wq, q_s, m_s, l_s, acc_s, kbuf, vbuf,
                 x_sem, w_sem, rail_send_sem, rail_recv_sem, sib_send_sem, sib_recv_sem, *score_refs):
    head_dim = q_s.shape[1]
    chunk = kbuf.shape[1]
    blocks = chunk // RB
    count = heads * blocks
    chips = cp_size // CORES
    me = lax.axis_index('cp')
    c = me // CORES
    b = me % CORES
    is_last = c == chips - 1
    above, below, sibling = me + CORES, me - CORES, c * CORES + (1 - b)
    has_above, has_below = c < chips - 1, c > 0
    s_refs = (score_refs[:count], score_refs[count:2 * count])
    x_refs = (score_refs[2 * count:3 * count], score_refs[3 * count:])

    def slot(n, r, s):
        return (n * (rounds + 1) + r) * 2 + s

    wk_copy = pltpu.make_async_copy(wk_hbm, wk, w_sem.at[0])
    wv_copy = pltpu.make_async_copy(wv_hbm, wv, w_sem.at[1])
    wq_copy = pltpu.make_async_copy(wq_hbm, wq_raw, w_sem.at[2])
    tiles = x_hbm.shape[0] // RB
    x_copies = [pltpu.make_async_copy(x_hbm.at[pl.ds(t * RB, RB)], xbuf.at[pl.ds(t * RB, RB)], x_sem.at[t]) for t in range(tiles)]
    x_copies[0].start()
    wk_copy.start()
    wv_copy.start()
    x_copies[1].start()

    m_s[...] = jnp.full_like(m_s, -jnp.inf)
    l_s[...] = jnp.zeros_like(l_s)
    acc_s[...] = jnp.zeros_like(acc_s)

    barrier = pltpu.get_barrier_semaphore()
    pl.semaphore_signal(barrier, inc=1, device_id={'cp': sibling}, device_id_type=pl.DeviceIdType.MESH)

    @pl.when(has_above)
    def _():
        pl.semaphore_signal(barrier, inc=1, device_id={'cp': above}, device_id_type=pl.DeviceIdType.MESH)

    @pl.when(has_below)
    def _():
        pl.semaphore_signal(barrier, inc=1, device_id={'cp': below}, device_id_type=pl.DeviceIdType.MESH)

    bufs = (kbuf, vbuf)

    def rail(n, r, kv):
        if n == 0:
            src, cond, target = slot(0, r - 1, 0), has_above & (c >= r - 1), above
        else:
            first = isinstance(r, int) and r == 1
            src = slot(1, 0, 0) if first else jnp.where(is_last, slot(0, r - 2, 0), slot(1, r - 1, 0))
            cond, target = has_below, below
        return cond, pltpu.make_async_remote_copy(
            src_ref=bufs[kv].at[src], dst_ref=bufs[kv].at[slot(n, r, 0)],
            send_sem=rail_send_sem.at[n, r - 1, kv], recv_sem=rail_recv_sem.at[n, r - 1, kv],
            device_id={'cp': target}, device_id_type=pl.DeviceIdType.MESH)

    def arrives(n, r):
        return c >= r if n == 0 else has_above

    def sib(n, r, kv):
        return pltpu.make_async_remote_copy(
            src_ref=bufs[kv].at[slot(n, r, 0)], dst_ref=bufs[kv].at[slot(n, r, 1)],
            send_sem=sib_send_sem.at[n, r, kv], recv_sem=sib_recv_sem.at[n, r, kv],
            device_id={'cp': sibling}, device_id_type=pl.DeviceIdType.MESH)

    own_push = ((b == 0) | is_last, b == 1)
    own_take = ((b == 1) | is_last, b == 0)

    def start_rail(n, r, kv):
        cond, copy = rail(n, r, kv)
        pl.when(cond)(copy.start)

    def relay(n, r, kv):
        @pl.when(arrives(n, r))
        def _():
            rail(n, r, kv)[1].wait_recv()
            sib(n, r, kv).start()
        if not isinstance(r, int) or r < rounds:
            start_rail(n, r + 1, kv)

    def project_kv(n):
        for tb in range(blocks):
            t = n * blocks + tb
            x_copies[t].wait()
            if t + 2 < tiles:
                x_copies[t + 2].start()
            elif t + 2 == tiles:
                wq_copy.start()
            rows = slice(t * RB, (t + 1) * RB)
            w_kv = jnp.concatenate([wk[...], wv[...]], axis=1)
            kv = jnp.dot(xbuf[rows, :], w_kv, preferred_element_type=jnp.float32).astype(jnp.bfloat16).astype(jnp.float32)
            k = rotate(kv[:, :head_dim].T, cos_ref[:, rows], sin_ref[:, rows])
            kbuf[slot(n, 0, 0), tb * RB:(tb + 1) * RB, :] = k.T.astype(jnp.bfloat16)
            vbuf[slot(n, 0, 0), :, tb * RB:(tb + 1) * RB] = kv[:, head_dim:].T.astype(jnp.bfloat16)

    wk_copy.wait()
    wv_copy.wait()
    project_kv(0)
    pl.semaphore_wait(barrier, 1 + has_above.astype(jnp.int32) + has_below.astype(jnp.int32))
    for n in range(2):
        if n == 1:
            project_kv(1)
        for kv in range(2):
            start_rail(n, 1, kv)

        @pl.when(own_push[n])
        def _(n=n):
            for kv in range(2):
                sib(n, 0, kv).start()

    wq_copy.wait()
    depth = wq.shape[0]
    span = wq_f32.shape[0] // heads

    def unpack(step, _):
        wq_f32[...] = wq_raw[pl.ds(pl.multiple_of(step * span * heads, span * heads), span * heads), :].astype(jnp.float32)
        for h in range(heads):
            wq[pl.ds(pl.multiple_of(step * span, span), span), h * head_dim:(h + 1) * head_dim] = wq_f32[pl.ds(h, span, stride=heads), :].astype(jnp.bfloat16)
        return 0
    lax.fori_loop(0, depth // span, unpack, 0)

    for t in range(tiles):
        rows = slice(t * RB, (t + 1) * RB)
        n, tb = t // blocks, t % blocks
        q = jnp.dot(xbuf[rows, :], wq[...], preferred_element_type=jnp.float32).astype(jnp.bfloat16).astype(jnp.float32)
        for h in range(heads):
            qh = rotate(q[:, h * head_dim:(h + 1) * head_dim].T, cos_ref[:, rows], sin_ref[:, rows]) * (head_dim ** -0.5)
            q_s[n, :, h * chunk + tb * RB:h * chunk + (tb + 1) * RB] = qh.astype(jnp.bfloat16)

    key_ids = lax.broadcasted_iota(jnp.int32, (RB, RB), 0)
    query_ids = lax.broadcasted_iota(jnp.int32, (RB, RB), 1)

    def mask_of(kind):
        return None if kind is None else (key_ids <= query_ids if kind == 'le' else key_ids > query_ids)

    def region(values, scores, parity):
        for i in range(count):
            cols = slice(i * RB, (i + 1) * RB)
            s_parts = scores.parts(i % blocks, blocks) if scores is not None else []
            v_parts = values.parts(i % blocks, blocks) if values is not None else []
            if values is not None:
                n = values.node
                m_old = m_s[n, :, cols]
                peak = jnp.maximum(m_old, jnp.broadcast_to(jnp.max(x_refs[parity][i][...], axis=0, keepdims=True), m_old.shape))
                scale = jnp.exp2((m_old - peak) * LOG2E)
                total = l_s[n, :, cols] * scale
            out = top = None
            s_row = v_row = 0
            for j in range(max(len(s_parts), len(v_parts))):
                if j < len(s_parts):
                    at, lo, hi, kind = s_parts[j]
                    top = score_part(q_s[scores.node, :, cols], kbuf[at, lo:hi, :], mask_of(kind), s_refs[1 - parity][i], s_row, top)
                    s_row += hi - lo
                if j < len(v_parts):
                    at, lo, hi, kind = v_parts[j]
                    total, part = value_part(s_refs[parity][i], v_row, vbuf[at, :, lo:hi], peak, total)
                    out = part if out is None else out + part
                    v_row += hi - lo
            if scores is not None:
                x_refs[1 - parity][i][...] = top
            if values is not None:
                m_s[n, :, cols] = peak
                l_s[n, :, cols] = total
                acc_s[n, :, cols] = (acc_s[n, :, cols].reshape(head_dim // SUB, SUB, RB) * scale[None]).reshape(head_dim, RB) + out

    def pair_slots(n, r):
        if n == 0:
            return [slot(0, r, s) for s in range(2)]
        return [jnp.where(is_last, slot(0, r - 1, s), slot(1, r, s)) for s in range(2)]

    one_n, two_n = 1 - b, b
    flip = (c > chips - 1 - rounds).astype(jnp.int32)
    high = jnp.where(is_last, slot(0, rounds - 1, 0), slot(1, rounds, 0))
    low = slot(0, rounds, 0)

    def edge_slots(node):
        return jnp.where(node == 0, low, high + flip), jnp.where(node == 0, low + 1, high + 1 - flip)

    def reaches(node):
        return (node == 1) | (c >= rounds)

    always = me != cp_size
    near, far = edge_slots(two_n), edge_slots(one_n)
    own_two = Step(two_n, diag=slot(0, 0, 0) + two_n * slot(1, 0, 0))
    own_one = Step(one_n, diag=slot(0, 0, 0) + one_n * slot(1, 0, 0), full=[slot(0, 0, 1) + one_n * slot(1, 0, 0)])
    edge_two = Step(two_n, edge=near[0], full=[near[1]])
    edge_one = Step(one_n, edge=far[0])

    def pair(n, r):
        return Step(n, full=pair_slots(n, r))

    def relay_both(r, kv):
        for n in range(2):
            relay(n, r, kv)

    def take(n, r, kv):
        cond = own_take[n] if isinstance(r, int) and r == 0 else arrives(n, r)
        pl.when(cond)(sib(n, r, kv).wait_recv)

    def run(step, following, parity, valid=None):
        pl.when(always if valid is None else valid)(functools.partial(region, step, following, parity))
        if valid is not None and following is not None:
            pl.when(jnp.logical_not(valid))(functools.partial(region, None, following, parity))

    region(None, own_two, 1)
    relay_both(1, 0)
    for n in range(2):
        take(n, 0, 0)
    run(own_two, own_one, 0)
    relay_both(1, 1)
    for n in range(2):
        take(n, 0, 1)
    take(0, 1, 0)
    run(own_one, pair(0, 1), 1)

    def round_of(r, after_low, after_high):
        relay_both(r + 1, 0)
        take(0, r, 1)
        take(1, r, 0)
        run(pair(0, r), pair(1, r), 0, c >= r)
        relay_both(r + 1, 1)
        take(1, r, 1)
        after_low()
        run(pair(1, r), after_high, 1)

    def middle(r, _):
        round_of(r, lambda: take(0, r + 1, 0), pair(0, r + 1))
        return 0
    lax.fori_loop(1, rounds - 1, middle, 0)

    def last_keys():
        for n in range(2):
            take(n, rounds, 0)
    round_of(rounds - 1, last_keys, edge_two)
    for n in range(2):
        take(n, rounds, 1)
    run(edge_two, edge_one, 0, reaches(two_n))
    run(edge_one, None, 1, reaches(one_n))

    def finish(h, _):
        for n in range(2):
            cols = pl.ds(pl.multiple_of(h * chunk, chunk), chunk)
            total = jnp.sum(l_s[n, :, cols], axis=0, keepdims=True)
            o_ref[n * chunk:(n + 1) * chunk, pl.ds(pl.multiple_of(h * head_dim, head_dim), head_dim)] = (acc_s[n, :, cols] / total).T.astype(jnp.bfloat16)
        return 0
    lax.fori_loop(0, heads, finish, 0)

    for n in range(2):
        for kv in range(2):
            for r in range(1, rounds + 1):
                cond, copy = rail(n, r, kv)
                pl.when(cond)(copy.wait_send)
                pl.when(arrives(n, r))(sib(n, r, kv).wait_send)
            pl.when(own_push[n])(sib(n, 0, kv).wait_send)


def out_kernel(band, o_ref, w_ref, y_ref):
    rows = pl.ds(pl.multiple_of(pl.program_id(0) * band, band), band)
    y_ref[...] = jnp.dot(o_ref[rows, :], w_ref[...], preferred_element_type=jnp.float32).astype(jnp.bfloat16)


def solution(mesh):
    cp_size = mesh.shape['cp']

    def device_step(hidden, w_q, w_k, w_v, w_o):
        rows, model_dim = hidden.shape
        chunk = rows // 2
        heads, head_dim = w_q.shape[1], w_q.shape[2]
        rounds = WINDOW // chunk // 2
        me = lax.axis_index('cp')
        chunk_ids = jnp.stack([me, 2 * cp_size - 1 - me])
        positions = (chunk_ids[:, None] * chunk + jnp.arange(chunk)[None, :]).reshape(rows)
        cos_part, sin_part = rope_tables(positions, head_dim)
        slots = 2 * (rounds + 1) * 2
        vmem = pl.BlockSpec(memory_space=pltpu.VMEM)
        hbm = pl.BlockSpec(memory_space=pltpu.HBM)
        attended = pl.pallas_call(
            functools.partial(fused_kernel, cp_size, rounds, heads),
            out_shape=jax.ShapeDtypeStruct((rows, heads * head_dim), jnp.bfloat16),
            in_specs=[vmem, vmem, hbm, hbm, hbm, hbm],
            out_specs=vmem,
            scratch_shapes=[
                pltpu.VMEM((rows, model_dim), jnp.bfloat16),
                pltpu.VMEM((model_dim, head_dim), jnp.bfloat16),
                pltpu.VMEM((model_dim, head_dim), jnp.bfloat16),
                pltpu.VMEM((model_dim * heads, head_dim), jnp.bfloat16),
                pltpu.VMEM((512 * heads, head_dim), jnp.float32),
                pltpu.VMEM((model_dim, heads * head_dim), jnp.bfloat16),
                pltpu.VMEM((2, head_dim, heads * chunk), jnp.bfloat16),
                pltpu.VMEM((2, SUB, heads * chunk), jnp.float32),
                pltpu.VMEM((2, SUB, heads * chunk), jnp.float32),
                pltpu.VMEM((2, head_dim, heads * chunk), jnp.float32),
                pltpu.VMEM((slots, chunk, head_dim), jnp.bfloat16),
                pltpu.VMEM((slots, head_dim, chunk), jnp.bfloat16),
                pltpu.SemaphoreType.DMA((rows // RB,)),
                pltpu.SemaphoreType.DMA((3,)),
                pltpu.SemaphoreType.DMA((2, rounds, 2)),
                pltpu.SemaphoreType.DMA((2, rounds, 2)),
                pltpu.SemaphoreType.DMA((2, rounds + 1, 2)),
                pltpu.SemaphoreType.DMA((2, rounds + 1, 2)),
            ] + [pltpu.VMEM((2 * chunk, RB), jnp.float32)] * (2 * heads * chunk // RB) + [pltpu.VMEM((SUB, RB), jnp.float32)] * (2 * heads * chunk // RB),
            compiler_params=pltpu.CompilerParams(collective_id=0, has_side_effects=True, vmem_limit_bytes=47 << 20),
        )(cos_part, sin_part, *(pltpu.with_memory_space_constraint(a, pltpu.HBM) for a in (hidden, w_k.reshape(model_dim, head_dim), w_v.reshape(model_dim, head_dim), w_q.reshape(model_dim * heads, head_dim))))
        band = 256
        return pl.pallas_call(
            functools.partial(out_kernel, band),
            out_shape=jax.ShapeDtypeStruct((rows, model_dim), jnp.bfloat16),
            grid=(rows // band,),
            in_specs=[vmem, vmem],
            out_specs=pl.BlockSpec((band, model_dim), lambda j: (j, 0)),
            compiler_params=pltpu.CompilerParams(vmem_limit_bytes=24 << 20),
        )(attended, w_o.reshape(heads * head_dim, model_dim))

    return jax.shard_map(device_step, mesh=mesh, in_specs=(P(('dp', 'cp'), None), P(), P(), P(), P()), out_specs=P(('dp', 'cp'), None), check_vma=False)
```

```python
import functools

import jax
import jax.numpy as jnp
from jax import lax
from jax.experimental import pallas as pl
from jax.experimental.pallas import tpu as pltpu
from jax.sharding import PartitionSpec as P

WINDOW = 4096
ROPE_BASE = 10000.0
LOG2E = 1.4426950408889634
RB = 256
SUB = 8
LANES = 128
CORES = 2


def rope_freqs(head_dim):
    half_dim = head_dim // 2
    inv_freq = 1.0 / (ROPE_BASE ** (jnp.arange(half_dim, dtype=jnp.float32) * (2.0 / head_dim)))
    return jnp.broadcast_to(inv_freq[:, None], (half_dim, LANES))


def rotate(values, cos_part, sin_part):
    half_dim = values.shape[0] // 2
    first, second = values[:half_dim], values[half_dim:]
    return jnp.concatenate([first * cos_part - second * sin_part, second * cos_part + first * sin_part], axis=0)


def score_part(q, keys, mask, s_ref, row, peak):
    scores = jnp.dot(keys, q, preferred_element_type=jnp.float32)
    if mask is not None:
        scores = jnp.where(mask, scores, -jnp.inf)
    rows = scores.shape[0]
    s_ref[row:row + rows, :] = scores
    top = jnp.max(scores.reshape(rows // SUB, SUB, RB), axis=0)
    return top if peak is None else jnp.maximum(peak, top)


def value_part(s_ref, row, vals, peak, total):
    rows = vals.shape[1]
    probs = jnp.exp2((s_ref[row:row + rows, :].reshape(rows // SUB, SUB, RB) - peak[None]) * LOG2E)
    total = total + jnp.sum(probs, axis=0)
    out = jnp.dot(vals, probs.reshape(rows, RB).astype(jnp.bfloat16), preferred_element_type=jnp.float32)
    return total, out


class Step:
    def __init__(self, node, full=(), diag=None, edge=None):
        self.node, self.full, self.diag, self.edge = node, full, diag, edge

    def parts(self, tb, blocks):
        found = []
        size = blocks * RB
        if self.diag is not None:
            if tb:
                found.append((self.diag, 0, tb * RB, None))
            found.append((self.diag, tb * RB, (tb + 1) * RB, 'le'))
        if self.edge is not None:
            found.append((self.edge, tb * RB, (tb + 1) * RB, 'gt'))
            if tb + 1 < blocks:
                found.append((self.edge, (tb + 1) * RB, size, None))
        for s in self.full:
            found.append((s, 0, size, None))
        return found


def fused_kernel(cp_size, rounds, heads, freq_ref, x_hbm, wk_hbm, wv_hbm, wq_hbm, wo_hbm, o_ref, wo_ref,
                 cos_ref, sin_ref, xbuf, wk, wv, wq_raw, wq_f32, wq, q_s, m_s, l_s, acc_s, kbuf, vbuf,
                 x_sem, w_sem, rail_send_sem, rail_recv_sem, sib_send_sem, sib_recv_sem, *score_refs):
    head_dim = q_s.shape[1]
    chunk = kbuf.shape[1]
    blocks = chunk // RB
    count = heads * blocks
    chips = cp_size // CORES
    me = lax.axis_index('cp')
    c = me // CORES
    b = me % CORES
    is_last = c == chips - 1
    above, below, sibling = me + CORES, me - CORES, c * CORES + (1 - b)
    has_above, has_below = c < chips - 1, c > 0
    s_refs = (score_refs[:count], score_refs[count:2 * count])
    x_refs = (score_refs[2 * count:3 * count], score_refs[3 * count:])

    def slot(n, r, s):
        return (n * (rounds + 1) + r) * 2 + s

    wk_copy = pltpu.make_async_copy(wk_hbm, wk, w_sem.at[0])
    wv_copy = pltpu.make_async_copy(wv_hbm, wv, w_sem.at[1])
    wq_copy = pltpu.make_async_copy(wq_hbm, wq_raw, w_sem.at[2])
    wo_copy = pltpu.make_async_copy(wo_hbm, wo_ref, w_sem.at[3])
    tiles = x_hbm.shape[0] // RB
    x_copies = [pltpu.make_async_copy(x_hbm.at[pl.ds(t * RB, RB)], xbuf.at[pl.ds(t * RB, RB)], x_sem.at[t]) for t in range(tiles)]
    x_copies[0].start()
    wk_copy.start()
    wv_copy.start()
    x_copies[1].start()

    barrier = pltpu.get_barrier_semaphore()
    pl.semaphore_signal(barrier, inc=1, device_id={'cp': sibling}, device_id_type=pl.DeviceIdType.MESH)

    @pl.when(has_above)
    def _():
        pl.semaphore_signal(barrier, inc=1, device_id={'cp': above}, device_id_type=pl.DeviceIdType.MESH)

    @pl.when(has_below)
    def _():
        pl.semaphore_signal(barrier, inc=1, device_id={'cp': below}, device_id_type=pl.DeviceIdType.MESH)

    lane_ids = lax.broadcasted_iota(jnp.int32, freq_ref.shape, 1)
    for n, chunk_id in enumerate((me, 2 * cp_size - 1 - me)):
        def table(j, _, n=n, chunk_id=chunk_id):
            angles = freq_ref[...] * (lane_ids + (chunk_id * chunk + j * LANES)).astype(jnp.float32)
            cols = pl.ds(pl.multiple_of(n * chunk + j * LANES, LANES), LANES)
            cos_ref[:, cols] = jnp.cos(angles)
            sin_ref[:, cols] = jnp.sin(angles)
            return 0
        lax.fori_loop(0, chunk // LANES, table, 0)

    bufs = (kbuf, vbuf)

    def rail(n, r, kv):
        if n == 0:
            src, cond, target = slot(0, r - 1, 0), has_above & (c >= r - 1), above
        else:
            first = isinstance(r, int) and r == 1
            src = slot(1, 0, 0) if first else jnp.where(is_last, slot(0, r - 2, 0), slot(1, r - 1, 0))
            cond, target = has_below, below
        return cond, pltpu.make_async_remote_copy(
            src_ref=bufs[kv].at[src], dst_ref=bufs[kv].at[slot(n, r, 0)],
            send_sem=rail_send_sem.at[n, r - 1, kv], recv_sem=rail_recv_sem.at[n, r - 1, kv],
            device_id={'cp': target}, device_id_type=pl.DeviceIdType.MESH)

    def arrives(n, r):
        return c >= r if n == 0 else has_above

    def sib(n, r, kv):
        return pltpu.make_async_remote_copy(
            src_ref=bufs[kv].at[slot(n, r, 0)], dst_ref=bufs[kv].at[slot(n, r, 1)],
            send_sem=sib_send_sem.at[n, r, kv], recv_sem=sib_recv_sem.at[n, r, kv],
            device_id={'cp': sibling}, device_id_type=pl.DeviceIdType.MESH)

    own_push = ((b == 0) | is_last, b == 1)
    own_take = ((b == 1) | is_last, b == 0)

    def start_rail(n, r, kv):
        cond, copy = rail(n, r, kv)
        pl.when(cond)(copy.start)

    def relay(n, r, kv):
        @pl.when(arrives(n, r))
        def _():
            rail(n, r, kv)[1].wait_recv()
            sib(n, r, kv).start()
        if not isinstance(r, int) or r < rounds:
            start_rail(n, r + 1, kv)

    def project_kv(n):
        for tb in range(blocks):
            t = n * blocks + tb
            x_copies[t].wait()
            if t + 2 < tiles:
                x_copies[t + 2].start()
            elif t + 2 == tiles:
                wq_copy.start()
            rows = slice(t * RB, (t + 1) * RB)
            w_kv = jnp.concatenate([wk[...], wv[...]], axis=1)
            kv = jnp.dot(xbuf[rows, :], w_kv, preferred_element_type=jnp.float32).astype(jnp.bfloat16).astype(jnp.float32)
            k = rotate(kv[:, :head_dim].T, cos_ref[:, rows], sin_ref[:, rows])
            kbuf[slot(n, 0, 0), tb * RB:(tb + 1) * RB, :] = k.T.astype(jnp.bfloat16)
            vbuf[slot(n, 0, 0), :, tb * RB:(tb + 1) * RB] = kv[:, head_dim:].T.astype(jnp.bfloat16)

    wk_copy.wait()
    wv_copy.wait()
    project_kv(0)
    pl.semaphore_wait(barrier, 1 + has_above.astype(jnp.int32) + has_below.astype(jnp.int32))
    for n in range(2):
        if n == 1:
            project_kv(1)
        for kv in range(2):
            start_rail(n, 1, kv)

        @pl.when(own_push[n])
        def _(n=n):
            for kv in range(2):
                sib(n, 0, kv).start()

    m_s[...] = jnp.full_like(m_s, -jnp.inf)
    l_s[...] = jnp.zeros_like(l_s)
    acc_s[...] = jnp.zeros_like(acc_s)

    wq_copy.wait()
    wo_copy.start()
    depth = wq.shape[0]
    span = wq_f32.shape[0] // heads

    def unpack(step, _):
        wq_f32[...] = wq_raw[pl.ds(pl.multiple_of(step * span * heads, span * heads), span * heads), :].astype(jnp.float32)
        for h in range(heads):
            wq[pl.ds(pl.multiple_of(step * span, span), span), h * head_dim:(h + 1) * head_dim] = wq_f32[pl.ds(h, span, stride=heads), :].astype(jnp.bfloat16)
        return 0
    lax.fori_loop(0, depth // span, unpack, 0)

    for t in range(tiles):
        rows = slice(t * RB, (t + 1) * RB)
        n, tb = t // blocks, t % blocks
        q = jnp.dot(xbuf[rows, :], wq[...], preferred_element_type=jnp.float32).astype(jnp.bfloat16).astype(jnp.float32)
        for h in range(heads):
            qh = rotate(q[:, h * head_dim:(h + 1) * head_dim].T, cos_ref[:, rows], sin_ref[:, rows]) * (head_dim ** -0.5)
            q_s[n, :, h * chunk + tb * RB:h * chunk + (tb + 1) * RB] = qh.astype(jnp.bfloat16)

    key_ids = lax.broadcasted_iota(jnp.int32, (RB, RB), 0)
    query_ids = lax.broadcasted_iota(jnp.int32, (RB, RB), 1)

    def mask_of(kind):
        return None if kind is None else (key_ids <= query_ids if kind == 'le' else key_ids > query_ids)

    def region(values, scores, parity):
        for i in range(count):
            cols = slice(i * RB, (i + 1) * RB)
            s_parts = scores.parts(i % blocks, blocks) if scores is not None else []
            v_parts = values.parts(i % blocks, blocks) if values is not None else []
            if values is not None:
                n = values.node
                m_old = m_s[n, :, cols]
                peak = jnp.maximum(m_old, jnp.broadcast_to(jnp.max(x_refs[parity][i][...], axis=0, keepdims=True), m_old.shape))
                scale = jnp.exp2((m_old - peak) * LOG2E)
                total = l_s[n, :, cols] * scale
            out = top = None
            s_row = v_row = 0
            for j in range(max(len(s_parts), len(v_parts))):
                if j < len(s_parts):
                    at, lo, hi, kind = s_parts[j]
                    top = score_part(q_s[scores.node, :, cols], kbuf[at, lo:hi, :], mask_of(kind), s_refs[1 - parity][i], s_row, top)
                    s_row += hi - lo
                if j < len(v_parts):
                    at, lo, hi, kind = v_parts[j]
                    total, part = value_part(s_refs[parity][i], v_row, vbuf[at, :, lo:hi], peak, total)
                    out = part if out is None else out + part
                    v_row += hi - lo
            if scores is not None:
                x_refs[1 - parity][i][...] = top
            if values is not None:
                m_s[n, :, cols] = peak
                l_s[n, :, cols] = total
                acc_s[n, :, cols] = (acc_s[n, :, cols].reshape(head_dim // SUB, SUB, RB) * scale[None]).reshape(head_dim, RB) + out

    def pair_slots(n, r):
        if n == 0:
            return [slot(0, r, s) for s in range(2)]
        return [jnp.where(is_last, slot(0, r - 1, s), slot(1, r, s)) for s in range(2)]

    one_n, two_n = 1 - b, b
    flip = (c > chips - 1 - rounds).astype(jnp.int32)
    high = jnp.where(is_last, slot(0, rounds - 1, 0), slot(1, rounds, 0))
    low = slot(0, rounds, 0)

    def edge_slots(node):
        return jnp.where(node == 0, low, high + flip), jnp.where(node == 0, low + 1, high + 1 - flip)

    def reaches(node):
        return (node == 1) | (c >= rounds)

    always = me != cp_size
    near, far = edge_slots(two_n), edge_slots(one_n)
    own_two = Step(two_n, diag=slot(0, 0, 0) + two_n * slot(1, 0, 0))
    own_one = Step(one_n, diag=slot(0, 0, 0) + one_n * slot(1, 0, 0), full=[slot(0, 0, 1) + one_n * slot(1, 0, 0)])
    edge_two = Step(two_n, edge=near[0], full=[near[1]])
    edge_one = Step(one_n, edge=far[0])

    def pair(n, r):
        return Step(n, full=pair_slots(n, r))

    def relay_both(r, kv):
        for n in range(2):
            relay(n, r, kv)

    def take(n, r, kv):
        cond = own_take[n] if isinstance(r, int) and r == 0 else arrives(n, r)
        pl.when(cond)(sib(n, r, kv).wait_recv)

    def run(step, following, parity, valid=None):
        pl.when(always if valid is None else valid)(functools.partial(region, step, following, parity))
        if valid is not None and following is not None:
            pl.when(jnp.logical_not(valid))(functools.partial(region, None, following, parity))

    region(None, own_two, 1)
    relay_both(1, 0)
    for n in range(2):
        take(n, 0, 0)
    run(own_two, own_one, 0)
    relay_both(1, 1)
    for n in range(2):
        take(n, 0, 1)
    take(0, 1, 0)
    run(own_one, pair(0, 1), 1)

    def round_of(r, after_low, after_high, last=False):
        relay_both(r + 1, 0)
        take(0, r, 1)
        take(1, r, 0)
        run(pair(0, r), pair(1, r), 0, c >= r)
        if last:
            relay(0, r + 1, 1)
        else:
            relay_both(r + 1, 1)
        take(1, r, 1)
        after_low()
        run(pair(1, r), after_high, 1)
        if last:
            relay(1, r + 1, 1)

    def middle(r, _):
        round_of(r, lambda: take(0, r + 1, 0), pair(0, r + 1))
        return 0
    lax.fori_loop(1, rounds - 1, middle, 0)

    def last_keys():
        for n in range(2):
            take(n, rounds, 0)
    round_of(rounds - 1, last_keys, edge_two)
    for n in range(2):
        take(n, rounds, 1)
    run(edge_two, edge_one, 0, reaches(two_n))
    run(edge_one, None, 1, reaches(one_n))

    def finish(h, _):
        for n in range(2):
            cols = pl.ds(pl.multiple_of(h * chunk, chunk), chunk)
            total = jnp.sum(l_s[n, :, cols], axis=0, keepdims=True)
            o_ref[n * chunk:(n + 1) * chunk, pl.ds(pl.multiple_of(h * head_dim, head_dim), head_dim)] = (acc_s[n, :, cols] / total).T.astype(jnp.bfloat16)
        return 0
    lax.fori_loop(0, heads, finish, 0)

    wo_copy.wait()
    for n in range(2):
        for kv in range(2):
            for r in range(1, rounds + 1):
                cond, copy = rail(n, r, kv)
                pl.when(cond)(copy.wait_send)
                pl.when(arrives(n, r))(sib(n, r, kv).wait_send)
            pl.when(own_push[n])(sib(n, 0, kv).wait_send)


def out_kernel(band, o_ref, w_ref, y_ref):
    rows = pl.ds(pl.multiple_of(pl.program_id(0) * band, band), band)
    y_ref[...] = jnp.dot(o_ref[rows, :], w_ref[...], preferred_element_type=jnp.float32).astype(jnp.bfloat16)


def solution(mesh):
    cp_size = mesh.shape['cp']

    def device_step(hidden, w_q, w_k, w_v, w_o):
        rows, model_dim = hidden.shape
        chunk = rows // 2
        heads, head_dim = w_q.shape[1], w_q.shape[2]
        rounds = WINDOW // chunk // 2
        slots = 2 * (rounds + 1) * 2
        vmem = pl.BlockSpec(memory_space=pltpu.VMEM)
        hbm = pl.BlockSpec(memory_space=pltpu.HBM)
        attended, w_out = pl.pallas_call(
            functools.partial(fused_kernel, cp_size, rounds, heads),
            out_shape=[jax.ShapeDtypeStruct((rows, heads * head_dim), jnp.bfloat16), jax.ShapeDtypeStruct((heads * head_dim, model_dim), jnp.bfloat16)],
            in_specs=[vmem, hbm, hbm, hbm, hbm, hbm],
            out_specs=[vmem, vmem],
            scratch_shapes=[
                pltpu.VMEM((head_dim // 2, rows), jnp.float32),
                pltpu.VMEM((head_dim // 2, rows), jnp.float32),
                pltpu.VMEM((rows, model_dim), jnp.bfloat16),
                pltpu.VMEM((model_dim, head_dim), jnp.bfloat16),
                pltpu.VMEM((model_dim, head_dim), jnp.bfloat16),
                pltpu.VMEM((model_dim * heads, head_dim), jnp.bfloat16),
                pltpu.VMEM((512 * heads, head_dim), jnp.float32),
                pltpu.VMEM((model_dim, heads * head_dim), jnp.bfloat16),
                pltpu.VMEM((2, head_dim, heads * chunk), jnp.bfloat16),
                pltpu.VMEM((2, SUB, heads * chunk), jnp.float32),
                pltpu.VMEM((2, SUB, heads * chunk), jnp.float32),
                pltpu.VMEM((2, head_dim, heads * chunk), jnp.float32),
                pltpu.VMEM((slots, chunk, head_dim), jnp.bfloat16),
                pltpu.VMEM((slots, head_dim, chunk), jnp.bfloat16),
                pltpu.SemaphoreType.DMA((rows // RB,)),
                pltpu.SemaphoreType.DMA((4,)),
                pltpu.SemaphoreType.DMA((2, rounds, 2)),
                pltpu.SemaphoreType.DMA((2, rounds, 2)),
                pltpu.SemaphoreType.DMA((2, rounds + 1, 2)),
                pltpu.SemaphoreType.DMA((2, rounds + 1, 2)),
            ] + [pltpu.VMEM((2 * chunk, RB), jnp.float32)] * (2 * heads * chunk // RB) + [pltpu.VMEM((SUB, RB), jnp.float32)] * (2 * heads * chunk // RB),
            compiler_params=pltpu.CompilerParams(collective_id=0, has_side_effects=True, vmem_limit_bytes=48 << 20),
        )(rope_freqs(head_dim), *(pltpu.with_memory_space_constraint(a, pltpu.HBM) for a in (hidden, w_k.reshape(model_dim, head_dim), w_v.reshape(model_dim, head_dim), w_q.reshape(model_dim * heads, head_dim), w_o.reshape(heads * head_dim, model_dim))))
        band = 256
        return pl.pallas_call(
            functools.partial(out_kernel, band),
            out_shape=jax.ShapeDtypeStruct((rows, model_dim), jnp.bfloat16),
            grid=(rows // band,),
            in_specs=[vmem, vmem],
            out_specs=pl.BlockSpec((band, model_dim), lambda j: (j, 0)),
            compiler_params=pltpu.CompilerParams(vmem_limit_bytes=24 << 20),
        )(attended, w_out)

    return jax.shard_map(device_step, mesh=mesh, in_specs=(P(('dp', 'cp'), None), P(), P(), P(), P()), out_specs=P(('dp', 'cp'), None), check_vma=False)
```

```python
import functools

import jax
import jax.numpy as jnp
from jax import lax
from jax.experimental import pallas as pl
from jax.experimental.pallas import tpu as pltpu
from jax.sharding import PartitionSpec as P

WINDOW = 4096
ROPE_BASE = 10000.0
LOG2E = 1.4426950408889634
RB = 256
SUB = 8
LANES = 128
CORES = 2


def rope_freqs(head_dim):
    half_dim = head_dim // 2
    inv_freq = 1.0 / (ROPE_BASE ** (jnp.arange(half_dim, dtype=jnp.float32) * (2.0 / head_dim)))
    return jnp.broadcast_to(inv_freq[:, None], (half_dim, LANES))


def rotate(values, cos_part, sin_part):
    half_dim = values.shape[0] // 2
    first, second = values[:half_dim], values[half_dim:]
    return jnp.concatenate([first * cos_part - second * sin_part, second * cos_part + first * sin_part], axis=0)


def score_part(q, keys, mask, s_ref, row, peak):
    scores = jnp.dot(keys, q, preferred_element_type=jnp.float32)
    if mask is not None:
        scores = jnp.where(mask, scores, -jnp.inf)
    rows = scores.shape[0]
    s_ref[row:row + rows, :] = scores
    top = jnp.max(scores.reshape(rows // SUB, SUB, RB), axis=0)
    return top if peak is None else jnp.maximum(peak, top)


def value_part(s_ref, row, vals, peak, total):
    rows = vals.shape[1]
    probs = jnp.exp2((s_ref[row:row + rows, :].reshape(rows // SUB, SUB, RB) - peak[None]) * LOG2E)
    total = total + jnp.sum(probs, axis=0)
    out = jnp.dot(vals, probs.reshape(rows, RB).astype(jnp.bfloat16), preferred_element_type=jnp.float32)
    return total, out


class Step:
    def __init__(self, node, full=(), diag=None, edge=None):
        self.node, self.full, self.diag, self.edge = node, full, diag, edge

    def parts(self, tb, blocks):
        found = []
        size = blocks * RB
        if self.diag is not None:
            if tb:
                found.append((self.diag, 0, tb * RB, None))
            found.append((self.diag, tb * RB, (tb + 1) * RB, 'le'))
        if self.edge is not None:
            found.append((self.edge, tb * RB, (tb + 1) * RB, 'gt'))
            if tb + 1 < blocks:
                found.append((self.edge, (tb + 1) * RB, size, None))
        for s in self.full:
            found.append((s, 0, size, None))
        return found


def fused_kernel(cp_size, rounds, heads, freq_ref, x_hbm, wk_hbm, wv_hbm, wq_hbm, wo_hbm, o_ref, wo_ref,
                 cos_ref, sin_ref, xbuf, wk, wv, wq_raw, wq_f32, wq, q_s, m_s, l_s, acc_s, kbuf, vbuf,
                 x_sem, w_sem, rail_send_sem, rail_recv_sem, sib_send_sem, sib_recv_sem, *score_refs):
    head_dim = q_s.shape[1]
    chunk = kbuf.shape[1]
    blocks = chunk // RB
    count = heads * blocks
    chips = cp_size // CORES
    me = lax.axis_index('cp')
    c = me // CORES
    b = me % CORES
    is_last = c == chips - 1
    above, below, sibling = me + CORES, me - CORES, c * CORES + (1 - b)
    has_above, has_below = c < chips - 1, c > 0
    s_refs = (score_refs[:count], score_refs[count:2 * count])
    x_refs = (score_refs[2 * count:3 * count], score_refs[3 * count:])

    def slot(n, r, s):
        return (n * (rounds + 1) + r) * 2 + s

    wk_copy = pltpu.make_async_copy(wk_hbm, wk, w_sem.at[0])
    wv_copy = pltpu.make_async_copy(wv_hbm, wv, w_sem.at[1])
    wq_copy = pltpu.make_async_copy(wq_hbm, wq_raw, w_sem.at[2])
    wo_copy = pltpu.make_async_copy(wo_hbm, wo_ref, w_sem.at[3])
    tiles = x_hbm.shape[0] // RB
    x_copies = [pltpu.make_async_copy(x_hbm.at[pl.ds(t * RB, RB)], xbuf.at[pl.ds(t * RB, RB)], x_sem.at[t]) for t in range(tiles)]
    x_copies[0].start()
    wk_copy.start()
    wv_copy.start()
    x_copies[1].start()

    barrier = pltpu.get_barrier_semaphore()
    pl.semaphore_signal(barrier, inc=1, device_id={'cp': sibling}, device_id_type=pl.DeviceIdType.MESH)

    @pl.when(has_above)
    def _():
        pl.semaphore_signal(barrier, inc=1, device_id={'cp': above}, device_id_type=pl.DeviceIdType.MESH)

    @pl.when(has_below)
    def _():
        pl.semaphore_signal(barrier, inc=1, device_id={'cp': below}, device_id_type=pl.DeviceIdType.MESH)

    lane_ids = lax.broadcasted_iota(jnp.int32, freq_ref.shape, 1)
    for n, chunk_id in enumerate((me, 2 * cp_size - 1 - me)):
        def table(j, _, n=n, chunk_id=chunk_id):
            angles = freq_ref[...] * (lane_ids + (chunk_id * chunk + j * LANES)).astype(jnp.float32)
            cols = pl.ds(pl.multiple_of(n * chunk + j * LANES, LANES), LANES)
            cos_ref[:, cols] = jnp.cos(angles)
            sin_ref[:, cols] = jnp.sin(angles)
            return 0
        lax.fori_loop(0, chunk // LANES, table, 0)

    bufs = (kbuf, vbuf)

    def rail(n, r, kv):
        if n == 0:
            src, cond, target = slot(0, r - 1, 0), has_above & (c >= r - 1), above
        else:
            first = isinstance(r, int) and r == 1
            src = slot(1, 0, 0) if first else jnp.where(is_last, slot(0, r - 2, 0), slot(1, r - 1, 0))
            cond, target = has_below, below
        return cond, pltpu.make_async_remote_copy(
            src_ref=bufs[kv].at[src], dst_ref=bufs[kv].at[slot(n, r, 0)],
            send_sem=rail_send_sem.at[n, r - 1, kv], recv_sem=rail_recv_sem.at[n, r - 1, kv],
            device_id={'cp': target}, device_id_type=pl.DeviceIdType.MESH)

    def arrives(n, r):
        return c >= r if n == 0 else has_above

    def sib(n, r, kv):
        return pltpu.make_async_remote_copy(
            src_ref=bufs[kv].at[slot(n, r, 0)], dst_ref=bufs[kv].at[slot(n, r, 1)],
            send_sem=sib_send_sem.at[n, r, kv], recv_sem=sib_recv_sem.at[n, r, kv],
            device_id={'cp': sibling}, device_id_type=pl.DeviceIdType.MESH)

    own_push = ((b == 0) | is_last, b == 1)
    own_take = ((b == 1) | is_last, b == 0)

    def start_rail(n, r, kv):
        cond, copy = rail(n, r, kv)
        pl.when(cond)(copy.start)

    def relay(n, r, kv):
        @pl.when(arrives(n, r))
        def _():
            rail(n, r, kv)[1].wait_recv()
            sib(n, r, kv).start()
        if not isinstance(r, int) or r < rounds:
            start_rail(n, r + 1, kv)

    def project_kv(n):
        for tb in range(blocks):
            t = n * blocks + tb
            x_copies[t].wait()
            if t + 2 < tiles:
                x_copies[t + 2].start()
            elif t + 2 == tiles:
                wq_copy.start()
            rows = slice(t * RB, (t + 1) * RB)
            w_kv = jnp.concatenate([wk[...], wv[...]], axis=1)
            kv = jnp.dot(xbuf[rows, :], w_kv, preferred_element_type=jnp.float32).astype(jnp.bfloat16).astype(jnp.float32)
            k = rotate(kv[:, :head_dim].T, cos_ref[:, rows], sin_ref[:, rows])
            kbuf[slot(n, 0, 0), tb * RB:(tb + 1) * RB, :] = k.T.astype(jnp.bfloat16)
            vbuf[slot(n, 0, 0), :, tb * RB:(tb + 1) * RB] = kv[:, head_dim:].T.astype(jnp.bfloat16)

    wk_copy.wait()
    wv_copy.wait()
    project_kv(0)
    pl.semaphore_wait(barrier, 1 + has_above.astype(jnp.int32) + has_below.astype(jnp.int32))
    for n in range(2):
        if n == 1:
            project_kv(1)
        for kv in range(2):
            start_rail(n, 1, kv)

        @pl.when(own_push[n])
        def _(n=n):
            for kv in range(2):
                sib(n, 0, kv).start()

    m_s[...] = jnp.full_like(m_s, -jnp.inf)
    l_s[...] = jnp.zeros_like(l_s)
    acc_s[...] = jnp.zeros_like(acc_s)

    wq_copy.wait()
    wo_copy.start()
    depth = wq.shape[0]
    span = wq_f32.shape[0] // heads

    def unpack(step, _):
        wq_f32[...] = wq_raw[pl.ds(pl.multiple_of(step * span * heads, span * heads), span * heads), :].astype(jnp.float32)
        for h in range(heads):
            wq[pl.ds(pl.multiple_of(step * span, span), span), h * head_dim:(h + 1) * head_dim] = wq_f32[pl.ds(h, span, stride=heads), :].astype(jnp.bfloat16)
        return 0
    lax.fori_loop(0, depth // span, unpack, 0)

    for t in range(tiles):
        rows = slice(t * RB, (t + 1) * RB)
        n, tb = t // blocks, t % blocks
        q = jnp.dot(xbuf[rows, :], wq[...], preferred_element_type=jnp.float32).astype(jnp.bfloat16).astype(jnp.float32)
        for h in range(heads):
            qh = rotate(q[:, h * head_dim:(h + 1) * head_dim].T, cos_ref[:, rows], sin_ref[:, rows]) * (head_dim ** -0.5)
            q_s[n, :, h * chunk + tb * RB:h * chunk + (tb + 1) * RB] = qh.astype(jnp.bfloat16)

    key_ids = lax.broadcasted_iota(jnp.int32, (RB, RB), 0)
    query_ids = lax.broadcasted_iota(jnp.int32, (RB, RB), 1)

    def mask_of(kind):
        return None if kind is None else (key_ids <= query_ids if kind == 'le' else key_ids > query_ids)

    def region(values, scores, parity):
        for i in range(count):
            cols = slice(i * RB, (i + 1) * RB)
            s_parts = scores.parts(i % blocks, blocks) if scores is not None else []
            v_parts = values.parts(i % blocks, blocks) if values is not None else []
            if values is not None:
                n = values.node
                m_old = m_s[n, :, cols]
                peak = jnp.maximum(m_old, jnp.broadcast_to(jnp.max(x_refs[parity][i][...], axis=0, keepdims=True), m_old.shape))
                scale = jnp.exp2((m_old - peak) * LOG2E)
                total = l_s[n, :, cols] * scale
            out = top = None
            s_row = v_row = 0
            for j in range(max(len(s_parts), len(v_parts))):
                if j < len(s_parts):
                    at, lo, hi, kind = s_parts[j]
                    top = score_part(q_s[scores.node, :, cols], kbuf[at, lo:hi, :], mask_of(kind), s_refs[1 - parity][i], s_row, top)
                    s_row += hi - lo
                if j < len(v_parts):
                    at, lo, hi, kind = v_parts[j]
                    total, part = value_part(s_refs[parity][i], v_row, vbuf[at, :, lo:hi], peak, total)
                    out = part if out is None else out + part
                    v_row += hi - lo
            if scores is not None:
                x_refs[1 - parity][i][...] = top
            if values is not None:
                m_s[n, :, cols] = peak
                l_s[n, :, cols] = total
                acc_s[n, :, cols] = (acc_s[n, :, cols].reshape(head_dim // SUB, SUB, RB) * scale[None]).reshape(head_dim, RB) + out

    def pair_slots(n, r):
        if n == 0:
            return [slot(0, r, s) for s in range(2)]
        return [jnp.where(is_last, slot(0, r - 1, s), slot(1, r, s)) for s in range(2)]

    one_n, two_n = 1 - b, b
    flip = (c > chips - 1 - rounds).astype(jnp.int32)
    high = jnp.where(is_last, slot(0, rounds - 1, 0), slot(1, rounds, 0))
    low = slot(0, rounds, 0)

    def edge_slots(node):
        return jnp.where(node == 0, low, high + flip), jnp.where(node == 0, low + 1, high + 1 - flip)

    def reaches(node):
        return (node == 1) | (c >= rounds)

    always = me != cp_size
    near, far = edge_slots(two_n), edge_slots(one_n)
    own_two = Step(two_n, diag=slot(0, 0, 0) + two_n * slot(1, 0, 0))
    own_one = Step(one_n, diag=slot(0, 0, 0) + one_n * slot(1, 0, 0), full=[slot(0, 0, 1) + one_n * slot(1, 0, 0)])
    edge_two = Step(two_n, edge=near[0], full=[near[1]])
    edge_one = Step(one_n, edge=far[0])

    def pair(n, r):
        return Step(n, full=pair_slots(n, r))

    def relay_both(r, kv):
        for n in range(2):
            relay(n, r, kv)

    def take(n, r, kv):
        cond = own_take[n] if isinstance(r, int) and r == 0 else arrives(n, r)
        pl.when(cond)(sib(n, r, kv).wait_recv)

    def run(step, following, parity, valid=None):
        pl.when(always if valid is None else valid)(functools.partial(region, step, following, parity))
        if valid is not None and following is not None:
            pl.when(jnp.logical_not(valid))(functools.partial(region, None, following, parity))

    region(None, own_two, 1)
    relay_both(1, 0)
    for n in range(2):
        take(n, 0, 0)
    run(own_two, own_one, 0)
    relay_both(1, 1)
    for n in range(2):
        take(n, 0, 1)
    take(0, 1, 0)
    run(own_one, pair(0, 1), 1)

    def round_of(r, after_low, after_high, last=False):
        relay_both(r + 1, 0)
        take(0, r, 1)
        take(1, r, 0)
        run(pair(0, r), pair(1, r), 0, c >= r)
        if last:
            relay(0, r + 1, 1)
        else:
            relay_both(r + 1, 1)
        take(1, r, 1)
        after_low()
        run(pair(1, r), after_high, 1)
        if last:
            relay(1, r + 1, 1)

    def middle(r, _):
        round_of(r, lambda: take(0, r + 1, 0), pair(0, r + 1))
        return 0
    lax.fori_loop(1, rounds - 1, middle, 0)

    def last_keys():
        for n in range(2):
            take(n, rounds, 0)
    round_of(rounds - 1, last_keys, edge_two)
    for n in range(2):
        take(n, rounds, 1)
    run(edge_two, edge_one, 0, reaches(two_n))
    run(edge_one, None, 1, reaches(one_n))

    def finish(h, _):
        for n in range(2):
            cols = pl.ds(pl.multiple_of(h * chunk, chunk), chunk)
            total = jnp.sum(l_s[n, :, cols], axis=0, keepdims=True)
            o_ref[n * chunk:(n + 1) * chunk, pl.ds(pl.multiple_of(h * head_dim, head_dim), head_dim)] = (acc_s[n, :, cols] / total).T.astype(jnp.bfloat16)
        return 0
    lax.fori_loop(0, heads, finish, 0)

    wo_copy.wait()
    for n in range(2):
        for kv in range(2):
            for r in range(1, rounds + 1):
                cond, copy = rail(n, r, kv)
                pl.when(cond)(copy.wait_send)
                pl.when(arrives(n, r))(sib(n, r, kv).wait_send)
            pl.when(own_push[n])(sib(n, 0, kv).wait_send)


def out_kernel(bands, halves, o_ref, w_ref, y_hbm, y_buf, y_sem):
    rows, cols = y_buf.shape[0] // bands, y_buf.shape[1] // halves
    copies = []
    for i in range(bands):
        for j in range(halves):
            at = (slice(i * rows, (i + 1) * rows), slice(j * cols, (j + 1) * cols))
            y_buf[at] = jnp.dot(o_ref[at[0], :], w_ref[:, at[1]], preferred_element_type=jnp.float32).astype(jnp.bfloat16)
            copies.append(pltpu.make_async_copy(y_buf.at[at], y_hbm.at[at], y_sem.at[i, j]))
            copies[-1].start()
    for copy in copies:
        copy.wait()


def solution(mesh):
    cp_size = mesh.shape['cp']

    def device_step(hidden, w_q, w_k, w_v, w_o):
        rows, model_dim = hidden.shape
        chunk = rows // 2
        heads, head_dim = w_q.shape[1], w_q.shape[2]
        rounds = WINDOW // chunk // 2
        slots = 2 * (rounds + 1) * 2
        vmem = pl.BlockSpec(memory_space=pltpu.VMEM)
        hbm = pl.BlockSpec(memory_space=pltpu.HBM)
        attended, w_out = pl.pallas_call(
            functools.partial(fused_kernel, cp_size, rounds, heads),
            out_shape=[jax.ShapeDtypeStruct((rows, heads * head_dim), jnp.bfloat16), jax.ShapeDtypeStruct((heads * head_dim, model_dim), jnp.bfloat16)],
            in_specs=[vmem, hbm, hbm, hbm, hbm, hbm],
            out_specs=[vmem, vmem],
            scratch_shapes=[
                pltpu.VMEM((head_dim // 2, rows), jnp.float32),
                pltpu.VMEM((head_dim // 2, rows), jnp.float32),
                pltpu.VMEM((rows, model_dim), jnp.bfloat16),
                pltpu.VMEM((model_dim, head_dim), jnp.bfloat16),
                pltpu.VMEM((model_dim, head_dim), jnp.bfloat16),
                pltpu.VMEM((model_dim * heads, head_dim), jnp.bfloat16),
                pltpu.VMEM((512 * heads, head_dim), jnp.float32),
                pltpu.VMEM((model_dim, heads * head_dim), jnp.bfloat16),
                pltpu.VMEM((2, head_dim, heads * chunk), jnp.bfloat16),
                pltpu.VMEM((2, SUB, heads * chunk), jnp.float32),
                pltpu.VMEM((2, SUB, heads * chunk), jnp.float32),
                pltpu.VMEM((2, head_dim, heads * chunk), jnp.float32),
                pltpu.VMEM((slots, chunk, head_dim), jnp.bfloat16),
                pltpu.VMEM((slots, head_dim, chunk), jnp.bfloat16),
                pltpu.SemaphoreType.DMA((rows // RB,)),
                pltpu.SemaphoreType.DMA((4,)),
                pltpu.SemaphoreType.DMA((2, rounds, 2)),
                pltpu.SemaphoreType.DMA((2, rounds, 2)),
                pltpu.SemaphoreType.DMA((2, rounds + 1, 2)),
                pltpu.SemaphoreType.DMA((2, rounds + 1, 2)),
            ] + [pltpu.VMEM((2 * chunk, RB), jnp.float32)] * (2 * heads * chunk // RB) + [pltpu.VMEM((SUB, RB), jnp.float32)] * (2 * heads * chunk // RB),
            compiler_params=pltpu.CompilerParams(collective_id=0, has_side_effects=True, vmem_limit_bytes=48 << 20),
        )(rope_freqs(head_dim), *(pltpu.with_memory_space_constraint(a, pltpu.HBM) for a in (hidden, w_k.reshape(model_dim, head_dim), w_v.reshape(model_dim, head_dim), w_q.reshape(model_dim * heads, head_dim), w_o.reshape(heads * head_dim, model_dim))))
        bands, halves = 4, 2
        return pl.pallas_call(
            functools.partial(out_kernel, bands, halves),
            out_shape=jax.ShapeDtypeStruct((rows, model_dim), jnp.bfloat16),
            in_specs=[vmem, vmem],
            out_specs=hbm,
            scratch_shapes=[pltpu.VMEM((rows, model_dim), jnp.bfloat16), pltpu.SemaphoreType.DMA((bands, halves))],
            compiler_params=pltpu.CompilerParams(vmem_limit_bytes=24 << 20),
        )(attended, w_out)

    return jax.shard_map(device_step, mesh=mesh, in_specs=(P(('dp', 'cp'), None), P(), P(), P(), P()), out_specs=P(('dp', 'cp'), None), check_vma=False)
```
